32 devices in a mesh: section: 4 (over x, core), dp: 8 (over z, y).
Axes of the slice: x: 2, y: 2, z: 4, core: 2. Of those that a mesh axis runs over, the one named last changes fastest.
Arguments:
- activations: bfloat16 [1536, 8, 4096], P('dp', 'section'), may hold values from -8 to 8
- damping: float32 [8], P('section'), may hold values from 0.1 to 1
Outputs:
- schur_inverse: float32 [256, 128, 128], P(('section', 'dp'))
- coupling: float32 [256, 128, 128], P(('section', 'dp'))
The draws below stay inside these ranges and needn't reach their ends.
All inputs are finite; a program needn't handle non-finite values.
Results may differ from the reference program's by a relative error of at most 0.0003.
Values may be sent and summed in bfloat16 or wider, within the bound.
A program may use at most 64 MiB of HBM per device.

```python
import math
from functools import partial
import jax
import jax.numpy as jnp
from jax import lax

D = 4096
B = 128
TOK_DEV = 192
L = 8
NB = 32
TOKENS = 1536


def column_filter():
    rows_idx = jnp.arange(B)[:, None]
    cols_idx = jnp.arange(B)[None, :]
    lag_power = jnp.maximum(rows_idx - cols_idx, 0).astype(jnp.float32)
    fresh_weight = jnp.where(cols_idx == 0, 1.0, jnp.sqrt(1.0 - 0.9 * 0.9)).astype(jnp.float32)
    weights = jnp.power(jnp.float32(0.9), lag_power) * fresh_weight
    return jnp.where(rows_idx >= cols_idx, weights, 0.0).astype(jnp.float32)


def draw_activations(key, part):
    shared_key = jax.random.fold_in(key, 11)
    fresh_key = jax.random.fold_in(key, 23)
    shard_key = jax.random.fold_in(key, 41)
    column_key = jax.random.fold_in(key, 53)
    shared_part = jax.random.normal(shared_key, (TOKENS, 1, D), jnp.float32)
    fresh_part = jax.random.normal(fresh_key, (TOKENS, L, D), jnp.float32)
    token_scale = jnp.ones((TOKENS, 1, 1), jnp.float32)
    shard_scale = jnp.exp(jax.random.uniform(shard_key, (TOKENS // TOK_DEV, 1, 1, 1), jnp.float32, -0.7, 0.7))
    column_scale = jnp.exp(jax.random.uniform(column_key, (1, L, D), jnp.float32, -0.7, 0.7))
    mixture = 0.75 * shared_part + 0.66 * fresh_part
    mixture = mixture.reshape(TOKENS, L, NB, B)
    mixture = jnp.einsum('tlgi,ji->tlgj', mixture, column_filter(), precision=lax.Precision.HIGHEST)
    mixture = mixture.reshape(TOKENS, L, D) * token_scale * column_scale
    mixture = (mixture.reshape(TOKENS // TOK_DEV, TOK_DEV, L, D) * shard_scale).reshape(TOKENS, L, D)
    return jnp.clip(mixture, -8.0, 8.0).astype(jnp.bfloat16)


def block_levels(key, shape, cuts, least, high):
    gain, own = 1.0, jax.random.fold_in(key, 6)
    for position, shards_of in cuts:
        heights = jnp.exp(jax.random.uniform(jax.random.fold_in(own, position), (shards_of,), jnp.float32, least / len(cuts), high / len(cuts)))
        gain = gain * jnp.repeat(heights, shape[position] // shards_of).reshape([-1 if axis == position else 1 for axis in range(len(shape))])
    return gain


def setup_inputs(seed: int = 0) -> dict:
    key_of = jax.random.split(jax.random.key(seed), 3)
    activations = draw_activations(jax.random.fold_in(key_of[2], 71), 0)
    damping = jnp.clip(jnp.exp(math.log(1.0) - 2.3025851 * jax.random.uniform(key_of[1], (L,), jnp.float32) ** block_levels(key_of[1], (L,), ((0, 4),), -0.2, 0.2)), 0.1, 1.0)
    return dict(activations=activations, damping=damping)


def layer_grams(activations, index):
    current = lax.dynamic_index_in_dim(activations, index, 1, keepdims=False)
    current = current.astype(jnp.float32).reshape(TOKENS, NB, B)
    later = jnp.minimum(index + 1, L - 1).astype(jnp.int32)
    following = lax.dynamic_index_in_dim(activations, later, 1, keepdims=False)
    following = following.astype(jnp.float32).reshape(TOKENS, NB, B)
    diagonal = jnp.einsum('tgb,tgc->gbc', current, current, precision=lax.Precision.HIGHEST) / TOKENS
    crossed = jnp.einsum('tgb,tgc->gbc', current, following, precision=lax.Precision.HIGHEST) / TOKENS
    return (diagonal, crossed)

def solve_block(system, right_side):
    factor = jnp.linalg.cholesky(system)
    return jax.scipy.linalg.cho_solve((factor, True), right_side)

def reference(activations, damping):
    diagonal_gram, cross_gram = lax.map(partial(layer_grams, activations), jnp.arange(L, dtype=jnp.int32))
    trace_mean = jnp.sum(jnp.trace(diagonal_gram, axis1=2, axis2=3), axis=1) / D
    identity = jnp.eye(B, dtype=jnp.float32)
    damped = diagonal_gram + (damping * trace_mean)[:, None, None, None] * identity
    final_mask = (jnp.arange(L) == L - 1)[:, None, None, None]
    following = jnp.concatenate([damped[1:], damped[:1]], axis=0)
    following = jnp.where(final_mask, identity, following)
    cross_gram = jnp.where(final_mask, jnp.zeros_like(cross_gram), cross_gram)
    damped = damped.reshape(L * NB, B, B)
    following = following.reshape(L * NB, B, B)
    cross_gram = cross_gram.reshape(L * NB, B, B)
    coupling_t = jax.vmap(solve_block)(following, jnp.swapaxes(cross_gram, 1, 2))
    schur = damped - jnp.matmul(cross_gram, coupling_t, precision=lax.Precision.HIGHEST)
    identities = jnp.broadcast_to(identity, schur.shape)
    schur_inverse = jax.vmap(solve_block)(schur, identities)
    return (schur_inverse, jnp.swapaxes(coupling_t, 1, 2))
```

```python
import functools

import jax
import jax.numpy as jnp
from jax import lax
from jax.experimental import pallas as pl
from jax.experimental.pallas import tpu as pltpu
from jax.sharding import PartitionSpec as P

B = 128
PANEL = 8


def passed_along(block, axis, distance):
    devices = range(lax.axis_size(axis))
    route = [(i - distance, i) for i in devices if i - distance in devices]
    return lax.ppermute(block, axis, route)


def invert_in_place(work, count, size):
    lane = lax.broadcasted_iota(jnp.int32, (count, size), 1)

    def step(_, carry):
        rows = [work[k * count : (k + 1) * count, :] for k in range(PANEL)]
        for k in range(PANEL):
            pivot = jnp.where(lane == k, 1.0, rows[k]) * (1.0 / rows[k][:, k : k + 1])
            for i in range(PANEL):
                if i != k:
                    rows[i] = jnp.where(lane == k, 0.0, rows[i]) - rows[i][:, k : k + 1] * pivot
            rows[k] = pivot
        for i in range(PANEL, size):
            row = work[i * count : (i + 1) * count, :]
            total = jnp.where(lane < PANEL, 0.0, row)
            for k in range(PANEL):
                total = total - row[:, k : k + 1] * rows[k]
            to = (i - PANEL) * count
            work[to : to + count, :] = pltpu.roll(total, size - PANEL, 1)
        for k in range(PANEL):
            to = (size - PANEL + k) * count
            work[to : to + count, :] = pltpu.roll(rows[k], size - PANEL, 1)
        return carry

    lax.fori_loop(0, size // PANEL, step, 0)


def blocks_kernel(count, tokens, levels, left, right, inverse, coupling, work, damped, cross):
    size = B
    identity = (
        lax.broadcasted_iota(jnp.int32, (size, size), 0)
        == lax.broadcasted_iota(jnp.int32, (size, size), 1)
    ).astype(jnp.float32)
    own_level, next_level, final = levels[0], levels[1], levels[2]
    exact = dict(preferred_element_type=jnp.float32, precision=lax.Precision.HIGHEST)

    for b in range(count):
        cols = slice(b * size, (b + 1) * size)
        both = jnp.concatenate([left[:, cols], right[:, cols]], axis=1)
        gram = lax.dot_general(
            both, both, (((0,), (0,)), ((), ())), preferred_element_type=jnp.float32
        ) / tokens
        damped[b] = gram[:size, :size] + own_level * identity
        cross[b] = jnp.where(final > 0.5, 0.0, gram[:size, size:])
        following = gram[size:, size:] + next_level * identity
        work[pl.ds(b, size, stride=count), :] = jnp.where(final > 0.5, identity, following)
    invert_in_place(work, count, size)
    for b in range(count):
        following_inverse = work[pl.ds(b, size, stride=count), :]
        coupled = jnp.dot(cross[b], following_inverse, **exact)
        coupling[b] = coupled
        taken = lax.dot_general(coupled, cross[b], (((1,), (1,)), ((), ())), **exact)
        work[pl.ds(b, size, stride=count), :] = damped[b] - taken
    invert_in_place(work, count, size)
    for b in range(count):
        inverse[b] = work[pl.ds(b, size, stride=count), :]


def local(activations, damping):
    token_rows, local_layers, model_width = activations.shape
    block_size = B
    blocks_layer = model_width // block_size
    group_size = lax.axis_size("dp")
    section_count = lax.axis_size("section")
    per_device = local_layers * blocks_layer // group_size
    tokens_all = token_rows * group_size
    owner_layer = lax.axis_index("dp") * per_device // blocks_layer

    squares = jnp.sum(jnp.square(activations.astype(jnp.float32)), axis=(0, 2))
    levels = damping * lax.psum(squares, "dp") / (tokens_all * model_width)
    levels = jnp.concatenate([levels, passed_along(levels[:1], "section", -1)])
    final_layer = jnp.logical_and(
        lax.axis_index("section") == section_count - 1, owner_layer == local_layers - 1
    )
    scalars = jnp.stack(
        [
            lax.dynamic_index_in_dim(levels, owner_layer, 0, keepdims=False),
            lax.dynamic_index_in_dim(levels, owner_layer + 1, 0, keepdims=False),
            final_layer.astype(jnp.float32),
        ]
    )

    flattened = activations.reshape(token_rows, local_layers * model_width)
    following_rows = passed_along(flattened[:, :model_width], "section", -1)
    next_layers = jnp.concatenate([flattened[:, model_width:], following_rows], axis=1)
    sent_pairs = (
        flattened.reshape(token_rows, group_size, per_device * block_size),
        next_layers.reshape(token_rows, group_size, per_device * block_size),
    )
    left_cols, right_cols = (
        lax.all_to_all(sent_pairs[0], "dp", split_axis=1, concat_axis=0, tiled=True),
        lax.all_to_all(sent_pairs[1], "dp", split_axis=1, concat_axis=0, tiled=True),
    )
    left_cols = left_cols.reshape(tokens_all, per_device * block_size)
    right_cols = right_cols.reshape(tokens_all, per_device * block_size)

    out = jax.ShapeDtypeStruct((per_device, block_size, block_size), jnp.float32)
    vmem = pl.BlockSpec(memory_space=pltpu.VMEM)
    return pl.pallas_call(
        functools.partial(blocks_kernel, per_device, tokens_all),
        out_shape=(out, out),
        in_specs=[pl.BlockSpec(memory_space=pltpu.SMEM), vmem, vmem],
        out_specs=(vmem, vmem),
        scratch_shapes=[
            pltpu.VMEM((block_size * per_device, block_size), jnp.float32),
            pltpu.VMEM((per_device, block_size, block_size), jnp.float32),
            pltpu.VMEM((per_device, block_size, block_size), jnp.float32),
        ],
        compiler_params=pltpu.CompilerParams(vmem_limit_bytes=48 * 1024 * 1024),
    )(scalars, left_cols, right_cols)


def solution(mesh):
    placed = (P("dp", "section", None), P("section"))
    return jax.shard_map(
        local,
        mesh=mesh,
        in_specs=placed,
        out_specs=(P(("section", "dp"), None, None), P(("section", "dp"), None, None)),
        check_vma=False,
    )
```

```python
import functools

import jax
import jax.numpy as jnp
from jax import lax
from jax.experimental import pallas as pl
from jax.experimental.pallas import tpu as pltpu
from jax.sharding import PartitionSpec as P

B = 128
PANEL = 8


def passed_along(block, axis, distance):
    devices = range(lax.axis_size(axis))
    route = [(i - distance, i) for i in devices if i - distance in devices]
    return lax.ppermute(block, axis, route)


def three_terms(value):
    high = value.astype(jnp.bfloat16).astype(jnp.float32)
    rest = value - high
    middle = rest.astype(jnp.bfloat16).astype(jnp.float32)
    return high, middle, rest - middle


def invert_in_place(work, panel, count, size):
    lane = lax.broadcasted_iota(jnp.int32, (count, size), 1)
    panel_lane = lax.broadcasted_iota(jnp.int32, (PANEL, size), 1)
    panel_row = lax.broadcasted_iota(jnp.int32, (PANEL, size), 0)
    full_lane = lax.broadcasted_iota(jnp.int32, (size, size), 1)
    full_row = lax.broadcasted_iota(jnp.int32, (size, size), 0)

    def step(s, carry):
        first = pl.multiple_of(s * PANEL, PANEL)
        rows, entries = [], []
        for k in range(PANEL):
            row = pltpu.roll(work[pl.ds(first + k, count, stride=size), :], size - first, 1)
            entries.append(
                [jnp.broadcast_to(row[:, j : j + 1], row.shape) for j in range(PANEL)]
            )
            rows.append(jnp.where(lane == k, 1.0, jnp.where(lane < PANEL, 0.0, row)))
        for k in range(PANEL):
            scale = 1.0 / entries[k][k]
            rows[k] = rows[k] * scale
            for j in range(k + 1, PANEL):
                entries[k][j] = entries[k][j] * scale
            for i in range(PANEL):
                if i != k:
                    factor = entries[i][k]
                    rows[i] = rows[i] - factor * rows[k]
                    for j in range(k + 1, PANEL):
                        entries[i][j] = entries[i][j] - factor * entries[k][j]
        for k in range(PANEL):
            panel[pl.ds(k, count, stride=PANEL), :] = pltpu.roll(rows[k], first, 1)
        local_lane = panel_lane - first
        in_panel = jnp.logical_and(local_lane >= 0, local_lane < PANEL)
        own = jnp.where(local_lane == panel_row, -1.0, 0.0)
        replaced = jnp.logical_or(
            jnp.logical_and(full_lane >= first, full_lane < first + PANEL),
            jnp.logical_and(full_row >= first, full_row < first + PANEL),
        )
        for b in range(count):
            old = work[pl.ds(b * size + first, PANEL), :]
            column = jnp.where(in_panel, own, jnp.where(local_lane < 0, -old, old))
            ch, cm, cl = three_terms(column)
            rh, rm, rl = three_terms(panel[b * PANEL : (b + 1) * PANEL, :])
            left = jnp.concatenate([ch, ch, ch, cm, cm, cl], axis=0).astype(jnp.bfloat16)
            right = jnp.concatenate([rh, rm, rl, rh, rm, rh], axis=0).astype(jnp.bfloat16)
            update = lax.dot_general(
                left, right, (((0,), (0,)), ((), ())), preferred_element_type=jnp.float32
            )
            at = slice(b * size, (b + 1) * size)
            work[at, :] = jnp.where(replaced, 0.0, work[at, :]) - update
        return carry

    lax.fori_loop(0, size // PANEL, step, 0)


def coupling_kernel(count, spread, tokens, levels, left, right, schur, coupling, work, panel, cross):
    size = B
    layers = count // spread
    identity = (
        lax.broadcasted_iota(jnp.int32, (size, size), 0)
        == lax.broadcasted_iota(jnp.int32, (size, size), 1)
    ).astype(jnp.float32)
    exact = dict(preferred_element_type=jnp.float32, precision=lax.Precision.HIGHEST)

    def cols(b):
        source, at = (left, b) if b < count else (right, b - count)
        return source[:, at * size : (at + 1) * size]

    for b in range(count):
        layer = b // spread
        both = jnp.concatenate([cols(b), cols(b + spread)], axis=1)
        gram = lax.dot_general(
            both, both, (((0,), (0,)), ((), ())), preferred_element_type=jnp.float32
        ) / tokens
        crossed = gram[:size, size:]
        following = gram[size:, size:] + levels[layer + 1] * identity
        if layer == layers - 1:
            final = levels[layers + 1] > 0.5
            crossed = jnp.where(final, 0.0, crossed)
            following = jnp.where(final, identity, following)
        schur[b] = gram[:size, :size] + levels[layer] * identity
        cross[b] = crossed
        work[b * size : (b + 1) * size, :] = following
    invert_in_place(work, panel, count, size)
    for b in range(count):
        coupled = jnp.dot(cross[b], work[b * size : (b + 1) * size, :], **exact)
        coupling[b] = coupled
        taken = lax.dot_general(coupled, cross[b], (((1,), (1,)), ((), ())), **exact)
        schur[b] = schur[b] - taken


def inverse_kernel(count, schur, inverse, panel):
    inverse[...] = schur[...]
    invert_in_place(inverse, panel, count, B)


def local(activations, damping):
    token_rows, local_layers, model_width = activations.shape
    block_size = B
    blocks_layer = model_width // block_size
    group_size = lax.axis_size("dp")
    section_count = lax.axis_size("section")
    per_device = local_layers * blocks_layer // group_size
    tokens_all = token_rows * group_size
    last_section = (lax.axis_index("section") == section_count - 1).astype(jnp.float32)

    squares = jnp.sum(jnp.square(activations.astype(jnp.float32)), axis=(0, 2))
    levels = damping * lax.psum(squares, "dp") / (tokens_all * model_width)
    levels = jnp.concatenate([levels, passed_along(levels[:1], "section", -1)])

    every_layer = per_device % local_layers == 0 and group_size % local_layers == 0
    if every_layer:
        spread = per_device // local_layers
        groups = group_size // local_layers
        sent = activations.reshape(
            token_rows, local_layers, groups, local_layers, spread * block_size
        )
        sent = sent.transpose(0, 3, 2, 1, 4).reshape(token_rows, group_size, -1)
        left_cols = lax.all_to_all(sent, "dp", split_axis=1, concat_axis=0, tiled=True)
        left_cols = left_cols.reshape(tokens_all, per_device * block_size)
        right_cols = passed_along(left_cols[:, : spread * block_size], "section", -1)
        scalars = jnp.concatenate([levels, last_section[None]])
    else:
        spread = per_device
        owner_layer = lax.axis_index("dp") * per_device // blocks_layer
        flattened = activations.reshape(token_rows, local_layers * model_width)
        following_rows = passed_along(flattened[:, :model_width], "section", -1)
        next_layers = jnp.concatenate([flattened[:, model_width:], following_rows], axis=1)
        left_cols, right_cols = (
            lax.all_to_all(
                sent.reshape(token_rows, group_size, -1), "dp", split_axis=1, concat_axis=0, tiled=True
            ).reshape(tokens_all, per_device * block_size)
            for sent in (flattened, next_layers)
        )
        last_layer = (owner_layer == local_layers - 1).astype(jnp.float32)
        scalars = jnp.concatenate(
            [lax.dynamic_slice(levels, (owner_layer,), (2,)), (last_section * last_layer)[None]]
        )

    blocks = (per_device, block_size, block_size)
    out = jax.ShapeDtypeStruct(blocks, jnp.float32)
    flat = jax.ShapeDtypeStruct((per_device * block_size, block_size), jnp.float32)
    vmem = pl.BlockSpec(memory_space=pltpu.VMEM)
    panel = pltpu.VMEM((per_device * PANEL, block_size), jnp.float32)
    schur, coupling = pl.pallas_call(
        functools.partial(coupling_kernel, per_device, spread, tokens_all),
        out_shape=(out, out),
        in_specs=[pl.BlockSpec(memory_space=pltpu.SMEM), vmem, vmem],
        out_specs=(vmem, vmem),
        scratch_shapes=[
            pltpu.VMEM(flat.shape, jnp.float32),
            panel,
            pltpu.VMEM(blocks, jnp.float32),
        ],
        compiler_params=pltpu.CompilerParams(vmem_limit_bytes=48 * 1024 * 1024),
    )(scalars, left_cols, right_cols)
    inverse = pl.pallas_call(
        functools.partial(inverse_kernel, per_device),
        out_shape=flat,
        in_specs=[vmem],
        out_specs=vmem,
        scratch_shapes=[panel],
        cost_estimate=pl.CostEstimate(
            flops=12 * per_device * block_size**3, bytes_accessed=40_000_000, transcendentals=0
        ),
    )(schur.reshape(flat.shape)).reshape(blocks)

    if every_layer:
        owners = [[h * groups + g for h in range(local_layers)] for g in range(groups)]
        inverse, coupling = (
            lax.all_to_all(
                x, "dp", split_axis=0, concat_axis=0, tiled=True, axis_index_groups=owners
            )
            for x in (inverse, coupling)
        )
    return inverse, coupling


def solution(mesh):
    placed = (P("dp", "section", None), P("section"))
    return jax.shard_map(
        local,
        mesh=mesh,
        in_specs=placed,
        out_specs=(P(("section", "dp"), None, None), P(("section", "dp"), None, None)),
        check_vma=False,
    )
```

```python
import functools

import jax
import jax.numpy as jnp
from jax import lax
from jax.experimental import pallas as pl
from jax.experimental.pallas import tpu as pltpu
from jax.sharding import PartitionSpec as P

B = 128
PANEL = 8


def passed_along(block, axis, distance):
    devices = range(lax.axis_size(axis))
    route = [(i - distance, i) for i in devices if i - distance in devices]
    return lax.ppermute(block, axis, route)


def handed_to_owners(blocks, layers, groups, spread):
    pieces = blocks.reshape(layers, spread, B, B)
    mine = lax.axis_index("dp") // groups
    kept = lax.dynamic_index_in_dim(pieces, mine, 0)
    result = jnp.broadcast_to(kept, pieces.shape)
    part = jnp.arange(layers).reshape(layers, 1, 1, 1)
    for shift in range(1, layers):
        route = [
            (h * groups + g, (h + shift) % layers * groups + g)
            for h in range(layers)
            for g in range(groups)
        ]
        sent = lax.dynamic_index_in_dim(pieces, (mine + shift) % layers, 0)
        came = lax.ppermute(sent, "dp", route)
        result = jnp.where(part == (mine - shift) % layers, came, result)
    return result.reshape(blocks.shape)


def three_terms(value):
    high = value.astype(jnp.bfloat16).astype(jnp.float32)
    rest = value - high
    middle = rest.astype(jnp.bfloat16).astype(jnp.float32)
    return high, middle, rest - middle


def invert_in_place(work, panel, count, size):
    lane = lax.broadcasted_iota(jnp.int32, (count, size), 1)
    panel_lane = lax.broadcasted_iota(jnp.int32, (PANEL, size), 1)
    panel_row = lax.broadcasted_iota(jnp.int32, (PANEL, size), 0)
    full_lane = lax.broadcasted_iota(jnp.int32, (size, size), 1)
    full_row = lax.broadcasted_iota(jnp.int32, (size, size), 0)

    def step(s, carry):
        first = pl.multiple_of(s * PANEL, PANEL)
        rows, entries = [], []
        for k in range(PANEL):
            row = pltpu.roll(work[pl.ds(first + k, count, stride=size), :], size - first, 1)
            entries.append(
                [jnp.broadcast_to(row[:, j : j + 1], row.shape) for j in range(PANEL)]
            )
            rows.append(jnp.where(lane == k, 1.0, jnp.where(lane < PANEL, 0.0, row)))
        for k in range(PANEL):
            scale = 1.0 / entries[k][k]
            rows[k] = rows[k] * scale
            for j in range(k + 1, PANEL):
                entries[k][j] = entries[k][j] * scale
            for i in range(PANEL):
                if i != k:
                    factor = entries[i][k]
                    rows[i] = rows[i] - factor * rows[k]
                    for j in range(k + 1, PANEL):
                        entries[i][j] = entries[i][j] - factor * entries[k][j]
        for k in range(PANEL):
            panel[pl.ds(k, count, stride=PANEL), :] = pltpu.roll(rows[k], first, 1)
        local_lane = panel_lane - first
        in_panel = jnp.logical_and(local_lane >= 0, local_lane < PANEL)
        own = jnp.where(local_lane == panel_row, -1.0, 0.0)
        replaced = jnp.logical_or(
            jnp.logical_and(full_lane >= first, full_lane < first + PANEL),
            jnp.logical_and(full_row >= first, full_row < first + PANEL),
        )
        for b in range(count):
            old = work[pl.ds(b * size + first, PANEL), :]
            column = jnp.where(in_panel, own, jnp.where(local_lane < 0, -old, old))
            ch, cm, cl = three_terms(column)
            rh, rm, rl = three_terms(panel[b * PANEL : (b + 1) * PANEL, :])
            left = jnp.concatenate([ch, ch, ch, cm, cm, cl], axis=0).astype(jnp.bfloat16)
            right = jnp.concatenate([rh, rm, rl, rh, rm, rh], axis=0).astype(jnp.bfloat16)
            update = lax.dot_general(
                left, right, (((0,), (0,)), ((), ())), preferred_element_type=jnp.float32
            )
            at = slice(b * size, (b + 1) * size)
            work[at, :] = jnp.where(replaced, 0.0, work[at, :]) - update
        return carry

    lax.fori_loop(0, size // PANEL, step, 0)


def coupling_kernel(count, spread, tokens, levels, left, right, schur, coupling, work, panel, cross):
    size = B
    layers = count // spread
    identity = (
        lax.broadcasted_iota(jnp.int32, (size, size), 0)
        == lax.broadcasted_iota(jnp.int32, (size, size), 1)
    ).astype(jnp.float32)
    exact = dict(preferred_element_type=jnp.float32, precision=lax.Precision.HIGHEST)

    def cols(b):
        source, at = (left, b) if b < count else (right, b - count)
        return source[:, at * size : (at + 1) * size]

    for b in range(count):
        layer = b // spread
        both = jnp.concatenate([cols(b), cols(b + spread)], axis=1)
        gram = lax.dot_general(
            both, both, (((0,), (0,)), ((), ())), preferred_element_type=jnp.float32
        ) / tokens
        crossed = gram[:size, size:]
        following = gram[size:, size:] + levels[layer + 1] * identity
        if layer == layers - 1:
            final = levels[layers + 1] > 0.5
            crossed = jnp.where(final, 0.0, crossed)
            following = jnp.where(final, identity, following)
        schur[b] = gram[:size, :size] + levels[layer] * identity
        cross[b] = crossed
        work[b * size : (b + 1) * size, :] = following
    invert_in_place(work, panel, count, size)
    for b in range(count):
        coupled = jnp.dot(cross[b], work[b * size : (b + 1) * size, :], **exact)
        coupling[b] = coupled
        taken = lax.dot_general(coupled, cross[b], (((1,), (1,)), ((), ())), **exact)
        schur[b] = schur[b] - taken


def inverse_kernel(count, schur, inverse, panel):
    inverse[...] = schur[...]
    invert_in_place(inverse, panel, count, B)


def local(activations, damping):
    token_rows, local_layers, model_width = activations.shape
    block_size = B
    blocks_layer = model_width // block_size
    group_size = lax.axis_size("dp")
    section_count = lax.axis_size("section")
    per_device = local_layers * blocks_layer // group_size
    tokens_all = token_rows * group_size
    last_section = (lax.axis_index("section") == section_count - 1).astype(jnp.float32)

    squares = jnp.sum(jnp.square(activations.astype(jnp.float32)), axis=(0, 2))
    levels = damping * lax.psum(squares, "dp") / (tokens_all * model_width)
    levels = jnp.concatenate([levels, passed_along(levels[:1], "section", -1)])

    every_layer = per_device % local_layers == 0 and group_size % local_layers == 0
    if every_layer:
        spread = per_device // local_layers
        groups = group_size // local_layers
        sent = activations.reshape(
            token_rows, local_layers, groups, local_layers, spread * block_size
        )
        sent = sent.transpose(0, 3, 2, 1, 4).reshape(token_rows, group_size, -1)
        left_cols = lax.all_to_all(sent, "dp", split_axis=1, concat_axis=0, tiled=True)
        left_cols = left_cols.reshape(tokens_all, per_device * block_size)
        right_cols = passed_along(left_cols[:, : spread * block_size], "section", -1)
        scalars = jnp.concatenate([levels, last_section[None]])
    else:
        spread = per_device
        owner_layer = lax.axis_index("dp") * per_device // blocks_layer
        flattened = activations.reshape(token_rows, local_layers * model_width)
        following_rows = passed_along(flattened[:, :model_width], "section", -1)
        next_layers = jnp.concatenate([flattened[:, model_width:], following_rows], axis=1)
        left_cols, right_cols = (
            lax.all_to_all(
                sent.reshape(token_rows, group_size, -1), "dp", split_axis=1, concat_axis=0, tiled=True
            ).reshape(tokens_all, per_device * block_size)
            for sent in (flattened, next_layers)
        )
        last_layer = (owner_layer == local_layers - 1).astype(jnp.float32)
        scalars = jnp.concatenate(
            [lax.dynamic_slice(levels, (owner_layer,), (2,)), (last_section * last_layer)[None]]
        )

    blocks = (per_device, block_size, block_size)
    out = jax.ShapeDtypeStruct(blocks, jnp.float32)
    flat = jax.ShapeDtypeStruct((per_device * block_size, block_size), jnp.float32)
    vmem = pl.BlockSpec(memory_space=pltpu.VMEM)
    panel = pltpu.VMEM((per_device * PANEL, block_size), jnp.float32)
    schur, coupling = pl.pallas_call(
        functools.partial(coupling_kernel, per_device, spread, tokens_all),
        out_shape=(out, out),
        in_specs=[pl.BlockSpec(memory_space=pltpu.SMEM), vmem, vmem],
        out_specs=(vmem, vmem),
        scratch_shapes=[
            pltpu.VMEM(flat.shape, jnp.float32),
            panel,
            pltpu.VMEM(blocks, jnp.float32),
        ],
        compiler_params=pltpu.CompilerParams(vmem_limit_bytes=48 * 1024 * 1024),
    )(scalars, left_cols, right_cols)
    inverse = pl.pallas_call(
        functools.partial(inverse_kernel, per_device),
        out_shape=flat,
        in_specs=[vmem],
        out_specs=vmem,
        scratch_shapes=[panel],
        cost_estimate=pl.CostEstimate(
            flops=12 * per_device * block_size**3, bytes_accessed=40_000_000, transcendentals=0
        ),
    )(schur.reshape(flat.shape)).reshape(blocks)

    if every_layer:
        inverse, coupling = (
            handed_to_owners(x, local_layers, groups, spread) for x in (inverse, coupling)
        )
    return inverse, coupling


def solution(mesh):
    placed = (P("dp", "section", None), P("section"))
    return jax.shard_map(
        local,
        mesh=mesh,
        in_specs=placed,
        out_specs=(P(("section", "dp"), None, None), P(("section", "dp"), None, None)),
        check_vma=False,
    )
```
